32 devices in a mesh: prow: 8 (over y, x, core), pcol: 4 (over z).
Axes of the slice: x: 2, y: 2, z: 4, core: 2. Of those that a mesh axis runs over, the one named last changes fastest.
Arguments:
- skeleton: float32 [2048, 32768], P('prow', 'pcol'), as said below
- pivots: int32 [2, 512], replicated, may hold values from 0 to 2047, as said below
Outputs:
- factored: float32 [2048, 32768], P('prow', 'pcol')
The draws below stay inside these ranges and needn't reach their ends.
Inputs may be any that keep to these rules, and one draw needn't show every extreme that they name: `pivots`: all 1024 entries are distinct. In each panel's list, entries g * 64 to (g + 1) * 64 - 1 are rows of the g-th block of 256 rows. `skeleton`: each step's pivot block D is invertible with a condition number below 10.
All inputs are finite; a program needn't handle non-finite values.
Results may differ from the reference program's by a relative error of at most 0.0001.
Values sent between devices are 32-bit elements; how exact they have to be, the bound alone decides.
No kernel may reach another device: no remote copies, remote signals or barrier semaphores. Data moves between devices by JAX's collectives and lax.ppermute only.
A program may use at most 128 MiB of HBM per device.

```python
import math
import jax
import jax.numpy as jnp
from jax import lax

ORDER = 32768
NB = 512
STEPS = 2
ROWS_DEV = 256
ROWS = 2048
N_PCOL = 4


def pivot_table(key):
    blocks = ROWS // ROWS_DEV
    share = NB // blocks
    keys = jax.random.split(key, blocks)
    orders = jax.vmap(lambda item: jax.random.permutation(item, ROWS_DEV))(keys)
    picked = orders[:, :STEPS * share].astype(jnp.int32).reshape(blocks, STEPS, share)
    picked = picked + (jnp.arange(blocks, dtype=jnp.int32) * ROWS_DEV)[:, None, None]
    return jnp.transpose(picked, (1, 0, 2)).reshape(STEPS, NB).astype(jnp.int32)


def draw_pivots(key, part):
    return pivot_table(jax.random.fold_in(key, 11))


def draw_skeleton(key, part):
    table = pivot_table(jax.random.fold_in(key, 11))
    width = STEPS * NB
    first_key = jax.random.fold_in(jax.random.fold_in(key, 23), 0)
    marks = (jnp.arange(ROWS, dtype=jnp.int32)[:, None] == table.reshape(-1)[None, :]).astype(jnp.float32)
    is_pivot = jnp.sum(marks, axis=1, keepdims=True)
    values = jax.random.normal(first_key, (ROWS, ORDER), jnp.float32)
    panel_scale = (1.0 - 0.75 * is_pivot) / math.sqrt(width)
    left_part = values[:, :width] * panel_scale + marks
    right_part = values[:, width:]
    return jnp.concatenate([left_part, right_part], axis=1)


def setup_inputs(seed: int = 0) -> dict:
    seeds = jax.random.split(jax.random.key(seed), 3)
    skeleton = draw_skeleton(jax.random.fold_in(seeds[2], 71), 0)
    pivots = draw_pivots(jax.random.fold_in(seeds[2], 71), 0)
    return {"skeleton": skeleton, "pivots": pivots}


def reference(skeleton, pivots):
    matrix = skeleton
    row_ids = jnp.arange(ROWS, dtype=jnp.int32)[:, None]
    column_ids = jnp.arange(ORDER, dtype=jnp.int32)[None, :]
    for step in range(STEPS):
        start = step * NB
        upper = jnp.take(matrix, pivots[step], axis=0)
        pivot_block = upper[:, start:start + NB]
        chosen = pivots[:step + 1].reshape(-1)
        active = jnp.all(row_ids != chosen[None, :], axis=1, keepdims=True)
        panel_cols = matrix[:, start:start + NB]
        solved = jnp.linalg.solve(pivot_block.T, panel_cols.T).T
        lower = jnp.where(active, solved, 0.0)
        update = jnp.dot(lower, upper, precision=lax.Precision.HIGHEST)
        matrix = matrix - jnp.where(column_ids >= start + NB, update, 0.0)
        kept = jnp.where(active, lower, matrix[:, start:start + NB])
        matrix = matrix.at[:, start:start + NB].set(kept)
    blocks_dev = ORDER // (N_PCOL * NB)
    shaped = matrix.reshape(ROWS, blocks_dev, N_PCOL, NB)
    return jnp.transpose(shaped, (0, 2, 1, 3)).reshape(ROWS, ORDER)
```

```python
import jax
import jax.numpy as jnp
from jax import lax
from jax.experimental import pallas as pl
from jax.experimental.pallas import tpu as pltpu
from jax.sharding import PartitionSpec as P

NB = 512
f32 = jnp.float32
bf16 = jnp.bfloat16
highest = lax.Precision.HIGHEST


def dot(a, b):
    return jnp.dot(a, b, preferred_element_type=f32)


def split2(x):
    hi = x.astype(bf16)
    return hi, (x - hi.astype(f32)).astype(bf16)


def dot3(a, b):
    ah, al = split2(a)
    bh, bl = split2(b)
    return dot(ah, bh) + (dot(ah, bl) + dot(al, bh))


def dot6(a, b):
    return jnp.dot(a, b, preferred_element_type=f32, precision=highest)


def select(onehot, x):
    y = x * 0.5
    hi = y.astype(bf16)
    rest = y - hi.astype(f32)
    mid = rest.astype(bf16)
    low = (rest - mid.astype(f32)).astype(bf16)
    return 2.0 * ((dot(onehot, hi) + dot(onehot, mid)) + dot(onehot, low))


def cost(flops, nbytes):
    return pl.CostEstimate(flops=int(flops), transcendentals=0, bytes_accessed=int(nbytes))


def params(n):
    return pltpu.CompilerParams(dimension_semantics=("arbitrary",) * n, vmem_limit_bytes=56 << 20)


def panel_rows(pidx, skeleton):
    rows = skeleton.shape[0]
    piv = pidx.shape[0]
    rest = rows - piv
    width = 2 * NB

    def body(idx_ref, x_ref, s_ref, st_ref, gp_ref, gn_ref):
        col = lax.broadcasted_iota(jnp.int32, (piv, rows), 1)
        sp = (col == idx_ref[...]).astype(f32)
        free = 1.0 - jnp.sum(sp, axis=0, keepdims=True)
        before = lax.broadcasted_iota(jnp.int32, (rows, rows), 0) < lax.broadcasted_iota(jnp.int32, (rows, rows), 1)
        rank = dot(jnp.broadcast_to(free, (8, rows)).astype(bf16), before.astype(f32).astype(bf16))[0:1]
        place = lax.broadcasted_iota(jnp.int32, (rest, rows), 0).astype(f32)
        sn = jnp.where(rank == place, free, 0.0)
        onehot = jnp.concatenate([sp, sn], axis=0)
        st_ref[...] = onehot.T.astype(bf16)
        s_ref[...] = onehot.astype(bf16)
        x = select(onehot.astype(bf16), x_ref[...])
        gp_ref[...] = x[0:piv]
        gn_ref[...] = x[piv:]

    full = lambda shape: pl.BlockSpec(shape, lambda i: (0, 0))
    shapes = [((rows, rows), bf16), ((rows, rows), bf16), ((piv, width), f32), ((rest, width), f32)]
    return pl.pallas_call(
        body,
        grid=(1,),
        in_specs=[full((piv, 1)), full((rows, width))],
        out_specs=[full(s) for s, _ in shapes],
        out_shape=[jax.ShapeDtypeStruct(s, d) for s, d in shapes],
        compiler_params=params(1),
        cost_estimate=cost(6 * rows * rows * width, 8 * rows * width),
        name="panel_rows",
    )(pidx, skeleton)


def pick(scalars, onehot, skeleton, k, devs, piv):
    rows, local = skeleton.shape
    per = local // NB // devs
    sizes = (piv, rows - piv)

    def body(sc_ref, s_ref, *refs):
        for i in range(per):
            x = select(s_ref[...], refs[i][...])
            refs[per][:, i * NB : (i + 1) * NB] = x[0:piv]
            refs[per + 1][:, i * NB : (i + 1) * NB] = x[piv:]

    block = lambda i: pl.BlockSpec((rows, NB), lambda _, sc: (0, lax.rem(sc[0] + k, devs) + devs * i))
    return pl.pallas_call(
        body,
        grid_spec=pltpu.PrefetchScalarGridSpec(
            num_scalar_prefetch=1,
            grid=(1,),
            in_specs=[pl.BlockSpec((rows, rows), lambda _, sc: (0, 0))] + [block(i) for i in range(per)],
            out_specs=[pl.BlockSpec((n, per * NB), lambda _, sc: (0, 0)) for n in sizes],
        ),
        out_shape=[jax.ShapeDtypeStruct((n, per * NB), f32) for n in sizes],
        compiler_params=params(1),
        cost_estimate=cost(6 * rows * rows * per * NB, 8 * rows * per * NB),
        name="pick",
    )(scalars, onehot, *[skeleton] * per)


def invert(d_ref, x_ref, r_ref):
    n = d_ref.shape[0]
    eye = lax.broadcasted_iota(jnp.int32, (n, n), 0) == lax.broadcasted_iota(jnp.int32, (n, n), 1)

    def total(v):
        return jnp.sum(jnp.sum(v, axis=0, keepdims=True), axis=1, keepdims=True)

    d = d_ref[...]
    size = jnp.max(jnp.max(jnp.abs(d), axis=0, keepdims=True), axis=1, keepdims=True)
    unit = 1.0 / size
    d = d * unit
    d_ref[...] = d
    dh = d.astype(bf16)
    power = lax.dot_general(dh, dh, (((1,), (1,)), ((), ())), preferred_element_type=f32)
    norm = jnp.sqrt(total(power * power))
    norms = [norm]
    for _ in range(3):
        ph = (power * (1.0 / norm)).astype(bf16)
        power = dot(ph, ph)
        norm = jnp.sqrt(total(power * power))
        norms.append(norm)
    bound = norms[-1]
    for value in reversed(norms[:-1]):
        bound = value * jnp.sqrt(bound)
    x_ref[...] = d.T * (1.7 / bound)

    def residual(product):
        r = jnp.where(eye, 1.0, 0.0) - product
        r_ref[...] = r
        return jnp.sum(r * r)

    def coarse(carry):
        x = x_ref[...]
        x_ref[...] = x + dot(x.astype(bf16), r_ref[...].astype(bf16))
        return carry[0] + 1, residual(dot(d_ref[...].astype(bf16), x_ref[...].astype(bf16)))

    def fine(carry):
        x = x_ref[...]
        x_ref[...] = x + dot3(x, r_ref[...])
        return carry[0] + 1, residual(dot3(d_ref[...], x_ref[...]))

    first = residual(dot(d_ref[...].astype(bf16), x_ref[...].astype(bf16)))
    done = lax.while_loop(lambda c: (c[1] > 1.0) & (c[0] < 24), coarse, (jnp.int32(0), first))
    start = residual(dot3(d_ref[...], x_ref[...]))
    lax.while_loop(lambda c: (c[1] > 4e-6) & (c[0] < 24), fine, (done[0] * 0, start))
    residual(dot6(d_ref[...], x_ref[...]))
    x = x_ref[...]
    x_ref[...] = (x + dot3(x, r_ref[...])) * unit


def natural(sc_ref, count, share):
    n = count * share
    at = lax.broadcasted_iota(jnp.int32, (share, n), 1) - lax.broadcasted_iota(jnp.int32, (share, n), 0)
    return jnp.concatenate([(at == sc_ref[2 + m] * share).astype(f32) for m in range(count)], axis=0).astype(bf16)


def place(x, onehot):
    y = x * 0.5
    hi = y.astype(bf16)
    rest = y - hi.astype(f32)
    mid = rest.astype(bf16)
    low = (rest - mid.astype(f32)).astype(bf16)
    return 2.0 * ((dot(hi, onehot) + dot(mid, onehot)) + dot(low, onehot))


def multipliers(scalars, blocks, panel_rest, share):
    rest = panel_rest.shape[0]
    half = share // 2
    width = 2 * NB
    count = len(blocks)

    def body(sc_ref, *refs):
        b_refs = refs[:count]
        pn_ref, l_ref, l0_ref, w0, w1, d_ref, x0, x1, r_ref, lp = refs[count:]

        @pl.when(sc_ref[0] != 0)
        def _():
            l_ref[...] = jnp.zeros_like(l_ref)
            l0_ref[...] = jnp.zeros_like(l0_ref)

        @pl.when(sc_ref[0] == 0)
        def _():
            for m in range(count):
                w0[m * share : (m + 1) * share, :] = b_refs[m][0:share, :]
                w1[m * share : (m + 1) * share, :] = b_refs[m][share : 2 * share, :]
            d_ref[...] = w0[:, 0:NB]
            invert(d_ref, x0, r_ref)
            lp[...] = dot3(w1[:, 0:NB], x0[...])
            d_ref[...] = w1[:, NB:width] - dot3(lp[...], w0[:, NB:width])
            invert(d_ref, x1, r_ref)
            l0 = dot3(pn_ref[:, 0:NB], x0[...])
            l1 = dot3(pn_ref[:, NB:width] - dot3(l0, w0[:, NB:width]), x1[...])
            l_ref[half:, 0:NB] = l0 - dot3(l1, lp[...])
            l_ref[half:, NB:width] = l1
            l_ref[0:half, 0:NB] = lp[0:half, :]
            l_ref[0:half, NB:width] = lp[half:share, :]
            back = natural(sc_ref, count, share)
            l0_ref[0:share, :] = place(lp[0:share, :], back)
            l0_ref[share:, :] = place(l0, back)

    full = lambda shape: pl.BlockSpec(shape, lambda i, sc: (0, 0))
    square = pltpu.VMEM((NB, NB), f32)
    return pl.pallas_call(
        body,
        grid_spec=pltpu.PrefetchScalarGridSpec(
            num_scalar_prefetch=1,
            grid=(1,),
            in_specs=[full((2 * share, width))] * count + [full((rest, width))],
            out_specs=[full((half + rest, width)), full((share + rest, NB))],
            scratch_shapes=[pltpu.VMEM((NB, width), f32)] * 2 + [square] * 5,
        ),
        out_shape=[jax.ShapeDtypeStruct((half + rest, width), f32), jax.ShapeDtypeStruct((share + rest, NB), f32)],
        compiler_params=params(1),
        cost_estimate=cost(30e9, 8 << 20),
        name="multipliers",
    )(scalars, *blocks, panel_rest)


def settle(scalars, parts, lower0, share, count):
    half = share // 2
    width = 2 * NB
    tall = lower0.shape[0]
    rest = tall - share

    def body(sc_ref, *refs):
        l0_ref, lh, fixed = refs[-3:]
        low = refs[0][...]
        for ref in refs[1:-3]:
            low = low + ref[...]
        fixed[...] = l0_ref[...]

        @pl.when(sc_ref[0] == 1)
        def _():
            fixed[share:, :] = place(low[half:, NB:width], natural(sc_ref, count, share))

        for n, piece in enumerate(split2(low)):
            at = n * tall
            lh[at : at + half, 0:NB] = piece[0:half, 0:NB]
            lh[at + half : at + share, 0:NB] = piece[0:half, NB:width]
            lh[at : at + share, NB:width] = jnp.zeros((share, NB), bf16)
            lh[at + share : at + tall, :] = piece[half:, :]

    full = lambda shape: pl.BlockSpec(shape, lambda i, sc: (0, 0))
    return pl.pallas_call(
        body,
        grid_spec=pltpu.PrefetchScalarGridSpec(
            num_scalar_prefetch=1,
            grid=(1,),
            in_specs=[full((half + rest, width))] * len(parts) + [full((tall, NB))],
            out_specs=[full((2 * tall, width)), full((tall, NB))],
        ),
        out_shape=[jax.ShapeDtypeStruct((2 * tall, width), bf16), jax.ShapeDtypeStruct((tall, NB), f32)],
        compiler_params=params(1),
        cost_estimate=cost(1e9, 4 * tall * width * (len(parts) + 2)),
        name="settle",
    )(scalars, *parts, lower0)


def came_from(sc, k, devs):
    return lax.rem(sc[0] + devs - k, devs)


def product(scalars, k, lh, fixed, blocks, share, devs):
    tall = fixed.shape[0]
    rest = tall - share
    piv = 2 * share
    width = 2 * NB
    total = blocks[0].shape[1]
    steps = total // NB
    count = len(blocks)
    piece = NB // 2

    def body(sc_ref, lh_ref, fixed_ref, *refs):
        b_refs = refs[:count]
        vp_ref, pn_ref, uh, ul = refs[count:]
        for j in range(2):
            cols = slice(j * piece, (j + 1) * piece)
            for m in range(count):
                hi, lo = split2(b_refs[m][:, cols])
                for t in range(2):
                    at = slice(t * NB + m * share, t * NB + (m + 1) * share)
                    uh[at, cols] = hi[t * share : (t + 1) * share]
                    ul[at, cols] = lo[t * share : (t + 1) * share]
            big = dot(lh_ref[...], uh[:, cols])
            prod = big[0:tall] + (big[tall:] + dot(lh_ref[0:tall, :], ul[:, cols]))
            vp_ref[0:share, cols] = b_refs[0][0:share, cols]
            vp_ref[share:piv, cols] = b_refs[0][share:piv, cols] - prod[0:share]
            pn_ref[:, cols] = prod[share:]

        @pl.when((pl.program_id(0) == 0) & (came_from(sc_ref, k, devs) == 0) & (sc_ref[0] == 0))
        def _():
            vp_ref[share:piv, :] = fixed_ref[0:share, :]

    full = lambda shape: pl.BlockSpec(shape, lambda i, sc: (0, 0))
    moving = lambda n: pl.BlockSpec((n, NB), lambda i, sc: (0, i))
    return pl.pallas_call(
        body,
        grid_spec=pltpu.PrefetchScalarGridSpec(
            num_scalar_prefetch=1,
            grid=(steps,),
            in_specs=[full((2 * tall, width)), full((tall, NB))] + [moving(piv)] * count,
            out_specs=[moving(piv), moving(rest)],
            scratch_shapes=[pltpu.VMEM((width, NB), bf16), pltpu.VMEM((width, NB), bf16)],
        ),
        out_shape=[jax.ShapeDtypeStruct((piv, total), f32), jax.ShapeDtypeStruct((rest, total), f32)],
        compiler_params=params(1),
        cost_estimate=cost(6 * tall * width * total, 4 * (width + piv + rest) * total),
        name="product",
    )(scalars, lh, fixed, *blocks)


def finish(scalars, k, st, fixed, done, prod, others, out, out_shape, devs):
    rows = st.shape[0]
    piv = done.shape[0]
    rest = rows - piv
    total = others.shape[1]
    tile = NB
    steps = total // tile

    def body(sc_ref, st_ref, fixed_ref, d_ref, p_ref, n_ref, *refs):
        o_ref, v = refs[-2:]
        v[0:piv, :] = d_ref[...]
        v[piv:, :] = n_ref[...] - p_ref[...]

        @pl.when((pl.program_id(0) == 0) & (came_from(sc_ref, k, devs) == 0) & (sc_ref[0] < 2))
        def _():
            v[piv:, :] = fixed_ref[piv // 2 :, :]

        o_ref[...] = select(st_ref[...], v[...])

    full = lambda shape: pl.BlockSpec(shape, lambda i, sc: (0, 0))
    moving = lambda n: pl.BlockSpec((n, tile), lambda i, sc: (0, i))
    operands = [st, fixed, done, prod, others]
    in_specs = [full((rows, rows)), full((fixed.shape[0], NB)), moving(piv), moving(rest), moving(rest)]
    aliases = {}
    if out is not None:
        aliases = {1 + len(operands): 0}
        operands.append(out)
        in_specs.append(pl.BlockSpec(memory_space=pl.ANY))
    return pl.pallas_call(
        body,
        grid_spec=pltpu.PrefetchScalarGridSpec(
            num_scalar_prefetch=1,
            grid=(steps,),
            in_specs=in_specs,
            out_specs=pl.BlockSpec((rows, tile), lambda i, sc: (0, came_from(sc, k, devs) * steps + i)),
            scratch_shapes=[pltpu.VMEM((rows, tile), f32)],
        ),
        out_shape=out_shape,
        input_output_aliases=aliases,
        compiler_params=params(1),
        cost_estimate=cost(6 * rows * rows * total, 4 * (rows + rest) * total),
        name="finish",
    )(scalars, *operands)


def across(x, size, move):
    return lax.ppermute(x, "prow", [(i, move(i)) for i in range(size)])


def gather_rows(x, size):
    blocks = [x]
    if size == 8:
        one = lambda i: i ^ (2 if i % 2 == 0 else 4)
        two = lambda i: i ^ (4 if i % 2 == 0 else 2)
        a = across(x, size, one)
        b = across(x, size, two)
        blocks += [a, b, across(a, size, two)]
    else:
        blocks += [across(x, size, lambda i, m=m: i ^ m) for m in range(2, size, 2)]
    return blocks + [across(block, size, lambda i: i ^ 1) for block in blocks]


def block_ids(row, size):
    even = row % 2 == 0
    if size == 8:
        ids = [row, jnp.where(even, row ^ 2, row ^ 4), jnp.where(even, row ^ 4, row ^ 2), row ^ 6]
        mate = row ^ 1
        ids += [mate, jnp.where(even, mate ^ 4, mate ^ 2), jnp.where(even, mate ^ 2, mate ^ 4), mate ^ 6]
        return ids
    ids = [row ^ m for m in range(0, size, 2)]
    return ids + [i ^ 1 for i in ids]


def on_device(skeleton, pivots):
    rows, local = skeleton.shape
    size = lax.axis_size("prow")
    devs = lax.axis_size("pcol")
    row = lax.axis_index("prow")
    col = lax.axis_index("pcol")
    share = NB // size
    scalars = jnp.stack([col, row] + block_ids(row, size)).astype(jnp.int32)
    own = lax.dynamic_slice_in_dim(pivots, row * share, share, axis=1) - row * rows
    pidx = own.reshape(2 * share, 1)
    onehot, st, panel_piv, panel_rest = panel_rows(pidx, skeleton)

    def shift(x, k):
        return lax.ppermute(x, "pcol", [(i, (i + k) % devs) for i in range(devs)])

    def send(x, pairs):
        return lax.ppermute(x, "pcol", pairs)

    order = rotations(devs)
    picked = {k: pick(scalars, onehot, skeleton, k, devs, 2 * share) for k in order + [0]}
    piv = {k: shift(picked[k][0], k) if k else picked[k][0] for k in [0] + order}
    panel = gather_rows(panel_piv, size)
    lower, lower0 = multipliers(scalars, panel, panel_rest, share)
    reach = devs // 2
    moved = send(lower, [(0, reach)])
    parts = [lower, moved]
    while reach > 1:
        reach //= 2
        direct = send(lower, [(0, reach)])
        onward = send(moved, [(i, i + reach) for i in range(2 * reach, devs, 2 * reach)])
        parts += [direct, onward]
        moved = moved + direct + onward if reach > 1 else moved
    rest = {k: shift(picked[k][1], k) if k else picked[k][1] for k in [0] + order}
    lh, fixed = settle(scalars, parts, lower0, share, len(panel))
    shape = jax.ShapeDtypeStruct((rows, local), f32)
    ready = {}
    for k in [0] + order:
        blocks = gather_rows(piv[k], size)
        ready[k] = product(scalars, k, lh, fixed, blocks, share, devs)
    out = None
    for k in [0] + order:
        out = finish(scalars, k, st, fixed, *ready[k], rest[k], out, shape, devs)
    return out


def rotations(devs):
    return sorted(range(1, devs), key=lambda k: (-min(k, devs - k), -k))


def solution(mesh):
    placed = (P("prow", "pcol"), P())
    return jax.shard_map(on_device, mesh=mesh, in_specs=placed, out_specs=P("prow", "pcol"), check_vma=False)
```

```python
import jax
import jax.numpy as jnp
from jax import lax
from jax.experimental import pallas as pl
from jax.experimental.pallas import tpu as pltpu
from jax.sharding import PartitionSpec as P

NB = 512
f32 = jnp.float32
bf16 = jnp.bfloat16
highest = lax.Precision.HIGHEST


def dot(a, b):
    return jnp.dot(a, b, preferred_element_type=f32)


def split2(x):
    hi = x.astype(bf16)
    return hi, (x - hi.astype(f32)).astype(bf16)


def dot3(a, b):
    ah, al = split2(a)
    bh, bl = split2(b)
    return dot(ah, bh) + (dot(ah, bl) + dot(al, bh))


def dot6(a, b):
    return jnp.dot(a, b, preferred_element_type=f32, precision=highest)


def select(onehot, x):
    y = x * 0.5
    hi = y.astype(bf16)
    rest = y - hi.astype(f32)
    mid = rest.astype(bf16)
    low = (rest - mid.astype(f32)).astype(bf16)
    return 2.0 * ((dot(onehot, hi) + dot(onehot, mid)) + dot(onehot, low))


def cost(flops, nbytes):
    return pl.CostEstimate(flops=int(flops), transcendentals=0, bytes_accessed=int(nbytes))


def params(n):
    return pltpu.CompilerParams(dimension_semantics=("arbitrary",) * n, vmem_limit_bytes=56 << 20)


def pick(scalars, onehot, skeleton, columns, piv, own=None):
    rows = skeleton.shape[0]
    rest = rows - piv
    per = len(columns)
    make = own is not None

    def order(own_ref, s_ref, st_ref):
        share = piv // 2
        line = lax.broadcasted_iota(jnp.int32, (rows, share), 0)
        chosen = jnp.concatenate([(line == own_ref[t : t + 1, :]).astype(f32) for t in range(2)], axis=1)
        sp = chosen.T
        free = 1.0 - jnp.sum(sp, axis=0, keepdims=True)
        before = lax.broadcasted_iota(jnp.int32, (rows, rows), 0) < lax.broadcasted_iota(jnp.int32, (rows, rows), 1)
        rank = dot(jnp.broadcast_to(free, (8, rows)).astype(bf16), before.astype(f32).astype(bf16))[0:1]
        place_of = lax.broadcasted_iota(jnp.int32, (rest, rows), 0).astype(f32)
        full_order = jnp.concatenate([sp, jnp.where(rank == place_of, free, 0.0)], axis=0)
        st_ref[...] = full_order.T.astype(bf16)
        s_ref[...] = full_order.astype(bf16)

    def body(sc_ref, s_in, *refs):
        piv_ref, rest_ref = refs[per : per + 2]
        if make:
            order(s_in, *refs[per + 2 :])
            s_in = refs[per + 2]
        for i in range(per):
            x = select(s_in[...], refs[i][...])
            piv_ref[:, i * NB : (i + 1) * NB] = x[0:piv]
            rest_ref[:, i * NB : (i + 1) * NB] = x[piv:]

    whole = lambda shape: pl.BlockSpec(shape, lambda _, sc: (0, 0))
    block = lambda at: pl.BlockSpec((rows, NB), lambda _, sc: (0, at(sc)))
    shapes = [((piv, per * NB), f32), ((rest, per * NB), f32)] + [((rows, rows), bf16)] * (2 if make else 0)
    source = own if make else onehot
    return pl.pallas_call(
        body,
        grid_spec=pltpu.PrefetchScalarGridSpec(
            num_scalar_prefetch=1,
            grid=(1,),
            in_specs=[whole(source.shape)] + [block(at) for at in columns],
            out_specs=[whole(x) for x, _ in shapes],
        ),
        out_shape=[jax.ShapeDtypeStruct(x, d) for x, d in shapes],
        compiler_params=params(1),
        cost_estimate=cost(6 * rows * rows * per * NB, 8 * rows * per * NB),
        name="pick",
    )(scalars, source, *[skeleton] * per)


def invert(d_ref, x_ref, r_ref):
    n = d_ref.shape[0]
    eye = lax.broadcasted_iota(jnp.int32, (n, n), 0) == lax.broadcasted_iota(jnp.int32, (n, n), 1)

    def total(v):
        return jnp.sum(jnp.sum(v, axis=0, keepdims=True), axis=1, keepdims=True)

    d = d_ref[...]
    size = jnp.max(jnp.max(jnp.abs(d), axis=0, keepdims=True), axis=1, keepdims=True)
    unit = 1.0 / size
    d = d * unit
    d_ref[...] = d
    dh = d.astype(bf16)
    power = lax.dot_general(dh, dh, (((1,), (1,)), ((), ())), preferred_element_type=f32)
    norm = jnp.sqrt(total(power * power))
    norms = [norm]
    for _ in range(3):
        ph = (power * (1.0 / norm)).astype(bf16)
        power = dot(ph, ph)
        norm = jnp.sqrt(total(power * power))
        norms.append(norm)
    bound = norms[-1]
    for value in reversed(norms[:-1]):
        bound = value * jnp.sqrt(bound)
    x_ref[...] = d.T * (1.7 / bound)

    def residual(product):
        r = jnp.where(eye, 1.0, 0.0) - product
        r_ref[...] = r
        return jnp.sum(r * r)

    def coarse(carry):
        x = x_ref[...]
        x_ref[...] = x + dot(x.astype(bf16), r_ref[...].astype(bf16))
        return carry[0] + 1, residual(dot(d_ref[...].astype(bf16), x_ref[...].astype(bf16)))

    def fine(carry):
        x = x_ref[...]
        x_ref[...] = x + dot3(x, r_ref[...])
        return carry[0] + 1, residual(dot3(d_ref[...], x_ref[...]))

    first = residual(dot(d_ref[...].astype(bf16), x_ref[...].astype(bf16)))
    done = lax.while_loop(lambda c: (c[1] > 1.0) & (c[0] < 24), coarse, (jnp.int32(0), first))
    start = residual(dot3(d_ref[...], x_ref[...]))
    lax.while_loop(lambda c: (c[1] > 4e-6) & (c[0] < 24), fine, (done[0] * 0, start))
    residual(dot6(d_ref[...], x_ref[...]))
    x = x_ref[...]
    x_ref[...] = (x + dot3(x, r_ref[...])) * unit


def natural(sc_ref, count, share):
    n = count * share
    at = lax.broadcasted_iota(jnp.int32, (share, n), 1) - lax.broadcasted_iota(jnp.int32, (share, n), 0)
    return jnp.concatenate([(at == sc_ref[2 + m] * share).astype(f32) for m in range(count)], axis=0).astype(bf16)


def place(x, onehot):
    y = x * 0.5
    hi = y.astype(bf16)
    rest = y - hi.astype(f32)
    mid = rest.astype(bf16)
    low = (rest - mid.astype(f32)).astype(bf16)
    return 2.0 * ((dot(hi, onehot) + dot(mid, onehot)) + dot(low, onehot))


def first_step(scalars, blocks, panel_rest, share):
    rest = panel_rest.shape[0]
    width = 2 * NB
    count = len(blocks)

    def body(sc_ref, *refs):
        b_refs = refs[:count]
        pn_ref, lp, d1, l0, bp, w0, w1, d_ref, x0, r_ref = refs[count:]

        @pl.when(sc_ref[0] == 0)
        def _():
            for m in range(count):
                w0[m * share : (m + 1) * share, :] = b_refs[m][0:share, :]
                w1[m * share : (m + 1) * share, :] = b_refs[m][share : 2 * share, :]
            d_ref[...] = w0[:, 0:NB]
            invert(d_ref, x0, r_ref)
            low = dot3(w1[:, 0:NB], x0[...])
            lp[...] = low
            d1[...] = w1[:, NB:width] - dot3(low, w0[:, NB:width])
            mine = dot3(pn_ref[:, 0:NB], x0[...])
            l0[...] = mine
            bp[...] = pn_ref[:, NB:width] - dot3(mine, w0[:, NB:width])

    full = lambda shape: pl.BlockSpec(shape, lambda i, sc: (0, 0))
    square = pltpu.VMEM((NB, NB), f32)
    shapes = [(NB, NB), (NB, NB), (rest, NB), (rest, NB)]
    return pl.pallas_call(
        body,
        grid_spec=pltpu.PrefetchScalarGridSpec(
            num_scalar_prefetch=1,
            grid=(1,),
            in_specs=[full((2 * share, width))] * count + [full((rest, width))],
            out_specs=[full(x) for x in shapes],
            scratch_shapes=[pltpu.VMEM((NB, width), f32)] * 2 + [square] * 3,
        ),
        out_shape=[jax.ShapeDtypeStruct(x, f32) for x in shapes],
        compiler_params=params(1),
        cost_estimate=cost(20e9, 8 << 20),
        name="first_step",
    )(scalars, *blocks, panel_rest)


def second_step(scalars, lp, d1, l0, bp, share):
    rest = l0.shape[0]
    half = share // 2
    width = 2 * NB
    count = NB // share

    def body(sc_ref, lp_ref, d1_ref, l0_in, bp_ref, l_ref, l0_ref, d_ref, x1, r_ref):
        @pl.when(sc_ref[0] != 0)
        def _():
            l_ref[...] = jnp.zeros_like(l_ref)
            l0_ref[...] = jnp.zeros_like(l0_ref)

        @pl.when(sc_ref[0] == 0)
        def _():
            d_ref[...] = d1_ref[...]
            invert(d_ref, x1, r_ref)
            l1 = dot3(bp_ref[...], x1[...])
            l_ref[half:, 0:NB] = l0_in[...] - dot3(l1, lp_ref[...])
            l_ref[half:, NB:width] = l1
            l_ref[0:half, 0:NB] = lp_ref[0:half, :]
            l_ref[0:half, NB:width] = lp_ref[half:share, :]
            back = natural(sc_ref, count, share)
            l0_ref[0:share, :] = place(lp_ref[0:share, :], back)
            l0_ref[share:, :] = place(l0_in[...], back)

    full = lambda shape: pl.BlockSpec(shape, lambda i, sc: (0, 0))
    square = pltpu.VMEM((NB, NB), f32)
    return pl.pallas_call(
        body,
        grid_spec=pltpu.PrefetchScalarGridSpec(
            num_scalar_prefetch=1,
            grid=(1,),
            in_specs=[full((NB, NB)), full((NB, NB)), full((rest, NB)), full((rest, NB))],
            out_specs=[full((half + rest, width)), full((share + rest, NB))],
            scratch_shapes=[square] * 3,
        ),
        out_shape=[jax.ShapeDtypeStruct((half + rest, width), f32), jax.ShapeDtypeStruct((share + rest, NB), f32)],
        compiler_params=params(1),
        cost_estimate=cost(15e9, 4 << 20),
        name="second_step",
    )(scalars, lp, d1, l0, bp)


def settle(scalars, parts, lower0, share, count):
    half = share // 2
    width = 2 * NB
    tall = lower0.shape[0]
    rest = tall - share

    def body(sc_ref, *refs):
        l0_ref, lh, fixed = refs[-3:]
        low = refs[0][...]
        for ref in refs[1:-3]:
            low = low + ref[...]
        fixed[...] = l0_ref[...]

        @pl.when(sc_ref[0] == 1)
        def _():
            fixed[share:, :] = place(low[half:, NB:width], natural(sc_ref, count, share))

        for n, piece in enumerate(split2(low)):
            at = n * tall
            lh[at : at + half, 0:NB] = piece[0:half, 0:NB]
            lh[at + half : at + share, 0:NB] = piece[0:half, NB:width]
            lh[at : at + share, NB:width] = jnp.zeros((share, NB), bf16)
            lh[at + share : at + tall, :] = piece[half:, :]

    full = lambda shape: pl.BlockSpec(shape, lambda i, sc: (0, 0))
    return pl.pallas_call(
        body,
        grid_spec=pltpu.PrefetchScalarGridSpec(
            num_scalar_prefetch=1,
            grid=(1,),
            in_specs=[full((half + rest, width))] * len(parts) + [full((tall, NB))],
            out_specs=[full((2 * tall, width)), full((tall, NB))],
        ),
        out_shape=[jax.ShapeDtypeStruct((2 * tall, width), bf16), jax.ShapeDtypeStruct((tall, NB), f32)],
        compiler_params=params(1),
        cost_estimate=cost(1e9, 4 * tall * width * (len(parts) + 2)),
        name="settle",
    )(scalars, *parts, lower0)


def came_from(sc, k):
    return sc[0] ^ k


def product(scalars, k, lh, fixed, blocks, share):
    tall = fixed.shape[0]
    rest = tall - share
    piv = 2 * share
    width = 2 * NB
    total = blocks[0].shape[1]
    count = len(blocks)
    piece = NB // 2
    tile = 2 * NB if total % (2 * NB) == 0 else NB
    steps = total // tile

    def body(sc_ref, lh_ref, fixed_ref, *refs):
        b_refs = refs[:count]
        vp_ref, pn_ref = refs[count:]
        for j in range(tile // piece):
            cols = slice(j * piece, (j + 1) * piece)
            raw = [ref[:, cols] for ref in b_refs]
            hi, lo = split2(jnp.concatenate([x[0:share] for x in raw] + [x[share:] for x in raw], axis=0))
            big = dot(lh_ref[...], hi)
            prod = big[0:tall] + (big[tall:] + dot(lh_ref[0:tall, :], lo))
            vp_ref[0:share, cols] = raw[0][0:share]
            vp_ref[share:piv, cols] = raw[0][share:] - prod[0:share]
            pn_ref[:, cols] = prod[share:]

        @pl.when((pl.program_id(0) == 0) & (came_from(sc_ref, k) == 0) & (sc_ref[0] == 0))
        def _():
            vp_ref[share:piv, 0:NB] = fixed_ref[0:share, :]

    full = lambda shape: pl.BlockSpec(shape, lambda i, sc: (0, 0))
    moving = lambda n: pl.BlockSpec((n, tile), lambda i, sc: (0, i))
    return pl.pallas_call(
        body,
        grid_spec=pltpu.PrefetchScalarGridSpec(
            num_scalar_prefetch=1,
            grid=(steps,),
            in_specs=[full((2 * tall, width)), full((tall, NB))] + [moving(piv)] * count,
            out_specs=[moving(piv), moving(rest)],
        ),
        out_shape=[jax.ShapeDtypeStruct((piv, total), f32), jax.ShapeDtypeStruct((rest, total), f32)],
        compiler_params=params(1),
        cost_estimate=cost(6 * tall * width * total, 4 * (width + piv + rest) * total),
        name="product",
    )(scalars, lh, fixed, *blocks)


def finish(scalars, k, st, fixed, done, prod, others, out, out_shape):
    rows = st.shape[0]
    piv = done.shape[0]
    rest = rows - piv
    total = others.shape[1]
    tile = 2 * NB if total % (2 * NB) == 0 else NB
    steps = total // tile
    piece = NB // 2

    def body(sc_ref, st_ref, fixed_ref, d_ref, p_ref, n_ref, *refs):
        o_ref = refs[-1]
        panel = (pl.program_id(0) == 0) & (came_from(sc_ref, k) == 0) & (sc_ref[0] < 2)
        for j in range(tile // piece):
            cols = slice(j * piece, (j + 1) * piece)
            low = n_ref[:, cols] - p_ref[:, cols]
            if (j + 1) * piece <= NB:
                low = jnp.where(panel, fixed_ref[piv // 2 :, cols], low)
            o_ref[:, cols] = select(st_ref[...], jnp.concatenate([d_ref[:, cols], low], axis=0))

    full = lambda shape: pl.BlockSpec(shape, lambda i, sc: (0, 0))
    moving = lambda n: pl.BlockSpec((n, tile), lambda i, sc: (0, i))
    operands = [st, fixed, done, prod, others]
    in_specs = [full((rows, rows)), full((fixed.shape[0], NB)), moving(piv), moving(rest), moving(rest)]
    aliases = {}
    if out is not None:
        aliases = {1 + len(operands): 0}
        operands.append(out)
        in_specs.append(pl.BlockSpec(memory_space=pl.ANY))
    return pl.pallas_call(
        body,
        grid_spec=pltpu.PrefetchScalarGridSpec(
            num_scalar_prefetch=1,
            grid=(steps,),
            in_specs=in_specs,
            out_specs=pl.BlockSpec((rows, tile), lambda i, sc: (0, came_from(sc, k) * steps + i)),
        ),
        out_shape=out_shape,
        input_output_aliases=aliases,
        compiler_params=params(1),
        cost_estimate=cost(6 * rows * rows * total, 4 * (rows + rest) * total),
        name="finish",
    )(scalars, *operands)


def across(x, size, move):
    return lax.ppermute(x, "prow", [(i, move(i)) for i in range(size)])


def gather_rows(x, size):
    blocks = [x]
    if size == 8:
        one = lambda i: i ^ (2 if i % 2 == 0 else 4)
        two = lambda i: i ^ (4 if i % 2 == 0 else 2)
        a = across(x, size, one)
        b = across(x, size, two)
        blocks += [a, b, across(a, size, two)]
    else:
        blocks += [across(x, size, lambda i, m=m: i ^ m) for m in range(2, size, 2)]
    return blocks + [across(block, size, lambda i: i ^ 1) for block in blocks]


def block_ids(row, size):
    even = row % 2 == 0
    if size == 8:
        ids = [row, jnp.where(even, row ^ 2, row ^ 4), jnp.where(even, row ^ 4, row ^ 2), row ^ 6]
        mate = row ^ 1
        ids += [mate, jnp.where(even, mate ^ 4, mate ^ 2), jnp.where(even, mate ^ 2, mate ^ 4), mate ^ 6]
        return ids
    ids = [row ^ m for m in range(0, size, 2)]
    return ids + [i ^ 1 for i in ids]


def on_device(skeleton, pivots):
    rows, local = skeleton.shape
    size = lax.axis_size("prow")
    devs = lax.axis_size("pcol")
    row = lax.axis_index("prow")
    col = lax.axis_index("pcol")
    share = NB // size
    scalars = jnp.stack([col, row] + block_ids(row, size)).astype(jnp.int32)
    own = lax.dynamic_slice_in_dim(pivots, row * share, share, axis=1) - row * rows

    def shift(x, k):
        return lax.ppermute(x, "pcol", [(i, i ^ k) for i in range(devs)])

    def send(x, pairs):
        return lax.ppermute(x, "pcol", pairs)

    order = rotations(devs)
    per = local // NB // devs
    towards = lambda k: [lambda sc, i=i: (sc[0] ^ k) + devs * i for i in range(per)]
    piv_rows = 2 * share
    first, *others = order
    *head, onehot, st = pick(scalars, None, skeleton, towards(first), piv_rows, own)
    picked = {first: head}
    for k in others + [0]:
        picked[k] = pick(scalars, onehot, skeleton, towards(k), piv_rows)
    panel_piv, panel_rest = pick(scalars, onehot, skeleton, [lambda sc: 0, lambda sc: 1], piv_rows)
    piv = {k: shift(picked[k][0], k) if k else picked[k][0] for k in [0] + order}
    panel = gather_rows(panel_piv, size)
    lp, d1, l0, bp = first_step(scalars, panel, panel_rest, share)
    lower, lower0 = second_step(scalars, lp, d1, l0, bp, share)
    reach = devs // 2
    moved = send(lower, [(0, reach)])
    parts = [lower, moved]
    while reach > 1:
        reach //= 2
        direct = send(lower, [(0, reach)])
        onward = send(moved, [(i, i + reach) for i in range(2 * reach, devs, 2 * reach)])
        parts += [direct, onward]
        moved = moved + direct + onward if reach > 1 else moved
    rest = {k: shift(picked[k][1], k) if k else picked[k][1] for k in [0] + order}
    lh, fixed = settle(scalars, parts, lower0, share, len(panel))
    shape = jax.ShapeDtypeStruct((rows, local), f32)
    ready = {}
    for k in [0] + order:
        blocks = gather_rows(piv[k], size)
        ready[k] = product(scalars, k, lh, fixed, blocks, share)
    out = None
    for k in [0] + order:
        out = finish(scalars, k, st, fixed, *ready[k], rest[k], out, shape)
    return out


def rotations(devs):
    return sorted(range(1, devs), key=lambda k: (k != devs - 1, k))


def solution(mesh):
    placed = (P("prow", "pcol"), P())
    return jax.shard_map(on_device, mesh=mesh, in_specs=placed, out_specs=P("prow", "pcol"), check_vma=False)
```

```python
import jax
import jax.numpy as jnp
from jax import lax
from jax.experimental import pallas as pl
from jax.experimental.pallas import tpu as pltpu
from jax.sharding import PartitionSpec as P

NB = 512
f32 = jnp.float32
bf16 = jnp.bfloat16
highest = lax.Precision.HIGHEST


def dot(a, b):
    return jnp.dot(a, b, preferred_element_type=f32)


def split2(x):
    hi = x.astype(bf16)
    return hi, (x - hi.astype(f32)).astype(bf16)


def dot3(a, b):
    ah, al = split2(a)
    bh, bl = split2(b)
    return dot(ah, bh) + (dot(ah, bl) + dot(al, bh))


def dot6(a, b):
    return jnp.dot(a, b, preferred_element_type=f32, precision=highest)


def select(onehot, x):
    y = x * 0.5
    hi = y.astype(bf16)
    rest = y - hi.astype(f32)
    mid = rest.astype(bf16)
    low = (rest - mid.astype(f32)).astype(bf16)
    return 2.0 * ((dot(onehot, hi) + dot(onehot, mid)) + dot(onehot, low))


def cost(flops, nbytes):
    return pl.CostEstimate(flops=int(flops), transcendentals=0, bytes_accessed=int(nbytes))


def params(n, mib=20):
    return pltpu.CompilerParams(dimension_semantics=("arbitrary",) * n, vmem_limit_bytes=mib << 20)


def pick(scalars, onehot, skeleton, columns, piv, own=None):
    rows = skeleton.shape[0]
    rest = rows - piv
    per = len(columns)
    make = own is not None

    def order(own_ref, s_ref, st_ref):
        share = piv // 2
        line = lax.broadcasted_iota(jnp.int32, (rows, share), 0)
        chosen = jnp.concatenate([(line == own_ref[t : t + 1, :]).astype(f32) for t in range(2)], axis=1)
        sp = chosen.T
        free = 1.0 - jnp.sum(sp, axis=0, keepdims=True)
        before = lax.broadcasted_iota(jnp.int32, (rows, rows), 0) < lax.broadcasted_iota(jnp.int32, (rows, rows), 1)
        rank = dot(jnp.broadcast_to(free, (8, rows)).astype(bf16), before.astype(f32).astype(bf16))[0:1]
        place_of = lax.broadcasted_iota(jnp.int32, (rest, rows), 0).astype(f32)
        full_order = jnp.concatenate([sp, jnp.where(rank == place_of, free, 0.0)], axis=0)
        st_ref[...] = full_order.T.astype(bf16)
        s_ref[...] = full_order.astype(bf16)

    def body(sc_ref, s_in, *refs):
        piv_ref, rest_ref = refs[per : per + 2]
        if make:
            order(s_in, *refs[per + 2 :])
            s_in = refs[per + 2]
        for i in range(per):
            x = select(s_in[...], refs[i][...])
            piv_ref[:, i * NB : (i + 1) * NB] = x[0:piv]
            rest_ref[:, i * NB : (i + 1) * NB] = x[piv:]

    whole = lambda shape: pl.BlockSpec(shape, lambda _, sc: (0, 0))
    block = lambda at: pl.BlockSpec((rows, NB), lambda _, sc: (0, at(sc)))
    shapes = [((piv, per * NB), f32), ((rest, per * NB), f32)] + [((rows, rows), bf16)] * (2 if make else 0)
    source = own if make else onehot
    return pl.pallas_call(
        body,
        grid_spec=pltpu.PrefetchScalarGridSpec(
            num_scalar_prefetch=1,
            grid=(1,),
            in_specs=[whole(source.shape)] + [block(at) for at in columns],
            out_specs=[whole(x) for x, _ in shapes],
        ),
        out_shape=[jax.ShapeDtypeStruct(x, d) for x, d in shapes],
        compiler_params=params(1),
        cost_estimate=cost(6 * rows * rows * per * NB, 8 * rows * per * NB),
        name="pick",
    )(scalars, source, *[skeleton] * per)


def invert(d_ref, x_ref, r_ref):
    n = d_ref.shape[0]
    eye = lax.broadcasted_iota(jnp.int32, (n, n), 0) == lax.broadcasted_iota(jnp.int32, (n, n), 1)

    def total(v):
        return jnp.sum(jnp.sum(v, axis=0, keepdims=True), axis=1, keepdims=True)

    d = d_ref[...]
    size = jnp.max(jnp.max(jnp.abs(d), axis=0, keepdims=True), axis=1, keepdims=True)
    unit = 1.0 / size
    d = d * unit
    d_ref[...] = d
    dh = d.astype(bf16)
    power = lax.dot_general(dh, dh, (((1,), (1,)), ((), ())), preferred_element_type=f32)
    norm = jnp.sqrt(total(power * power))
    norms = [norm]
    for _ in range(3):
        ph = (power * (1.0 / norm)).astype(bf16)
        power = dot(ph, ph)
        norm = jnp.sqrt(total(power * power))
        norms.append(norm)
    bound = norms[-1]
    for value in reversed(norms[:-1]):
        bound = value * jnp.sqrt(bound)
    x_ref[...] = d.T * (1.7 / bound)

    def residual(product):
        r = jnp.where(eye, 1.0, 0.0) - product
        r_ref[...] = r
        return jnp.sum(r * r)

    def coarse(carry):
        x = x_ref[...]
        x_ref[...] = x + dot(x.astype(bf16), r_ref[...].astype(bf16))
        return carry[0] + 1, residual(dot(d_ref[...].astype(bf16), x_ref[...].astype(bf16)))

    def fine(carry):
        x = x_ref[...]
        x_ref[...] = x + dot3(x, r_ref[...])
        return carry[0] + 1, residual(dot3(d_ref[...], x_ref[...]))

    first = residual(dot(d_ref[...].astype(bf16), x_ref[...].astype(bf16)))
    done = lax.while_loop(lambda c: (c[1] > 1.0) & (c[0] < 24), coarse, (jnp.int32(0), first))
    start = residual(dot3(d_ref[...], x_ref[...]))
    lax.while_loop(lambda c: (c[1] > 4e-6) & (c[0] < 24), fine, (done[0] * 0, start))
    residual(dot6(d_ref[...], x_ref[...]))
    x = x_ref[...]
    x_ref[...] = (x + dot3(x, r_ref[...])) * unit


def natural(sc_ref, count, share):
    n = count * share
    at = lax.broadcasted_iota(jnp.int32, (share, n), 1) - lax.broadcasted_iota(jnp.int32, (share, n), 0)
    return jnp.concatenate([(at == sc_ref[2 + m] * share).astype(f32) for m in range(count)], axis=0).astype(bf16)


def place(x, onehot):
    y = x * 0.5
    hi = y.astype(bf16)
    rest = y - hi.astype(f32)
    mid = rest.astype(bf16)
    low = (rest - mid.astype(f32)).astype(bf16)
    return 2.0 * ((dot(hi, onehot) + dot(mid, onehot)) + dot(low, onehot))


def first_step(scalars, blocks, panel_rest, share):
    rest = panel_rest.shape[0]
    width = 2 * NB
    count = len(blocks)

    def body(sc_ref, *refs):
        b_refs = refs[:count]
        pn_ref, lp, d1, l0, bp, w0, w1, d_ref, x0, r_ref = refs[count:]

        @pl.when(sc_ref[0] == 0)
        def _():
            for m in range(count):
                w0[m * share : (m + 1) * share, :] = b_refs[m][0:share, :]
                w1[m * share : (m + 1) * share, :] = b_refs[m][share : 2 * share, :]
            d_ref[...] = w0[:, 0:NB]
            invert(d_ref, x0, r_ref)
            low = dot3(w1[:, 0:NB], x0[...])
            lp[...] = low
            d1[...] = w1[:, NB:width] - dot3(low, w0[:, NB:width])
            mine = dot3(pn_ref[:, 0:NB], x0[...])
            l0[...] = mine
            bp[...] = pn_ref[:, NB:width] - dot3(mine, w0[:, NB:width])

    full = lambda shape: pl.BlockSpec(shape, lambda i, sc: (0, 0))
    square = pltpu.VMEM((NB, NB), f32)
    shapes = [(NB, NB), (NB, NB), (rest, NB), (rest, NB)]
    return pl.pallas_call(
        body,
        grid_spec=pltpu.PrefetchScalarGridSpec(
            num_scalar_prefetch=1,
            grid=(1,),
            in_specs=[full((2 * share, width))] * count + [full((rest, width))],
            out_specs=[full(x) for x in shapes],
            scratch_shapes=[pltpu.VMEM((NB, width), f32)] * 2 + [square] * 3,
        ),
        out_shape=[jax.ShapeDtypeStruct(x, f32) for x in shapes],
        compiler_params=params(1, 32),
        cost_estimate=cost(20e9, 8 << 20),
        name="first_step",
    )(scalars, *blocks, panel_rest)


def second_step(scalars, lp, d1, l0, bp, share):
    rest = l0.shape[0]
    half = share // 2
    width = 2 * NB
    count = NB // share

    def body(sc_ref, lp_ref, d1_ref, l0_in, bp_ref, l_ref, l0_ref, d_ref, x1, r_ref):
        @pl.when(sc_ref[0] != 0)
        def _():
            l_ref[...] = jnp.zeros_like(l_ref)
            l0_ref[...] = jnp.zeros_like(l0_ref)

        @pl.when(sc_ref[0] == 0)
        def _():
            d_ref[...] = d1_ref[...]
            invert(d_ref, x1, r_ref)
            l1 = dot3(bp_ref[...], x1[...])
            l_ref[half:, 0:NB] = l0_in[...] - dot3(l1, lp_ref[...])
            l_ref[half:, NB:width] = l1
            l_ref[0:half, 0:NB] = lp_ref[0:half, :]
            l_ref[0:half, NB:width] = lp_ref[half:share, :]
            back = natural(sc_ref, count, share)
            l0_ref[0:share, :] = place(lp_ref[0:share, :], back)
            l0_ref[share:, :] = place(l0_in[...], back)

    full = lambda shape: pl.BlockSpec(shape, lambda i, sc: (0, 0))
    square = pltpu.VMEM((NB, NB), f32)
    return pl.pallas_call(
        body,
        grid_spec=pltpu.PrefetchScalarGridSpec(
            num_scalar_prefetch=1,
            grid=(1,),
            in_specs=[full((NB, NB)), full((NB, NB)), full((rest, NB)), full((rest, NB))],
            out_specs=[full((half + rest, width)), full((share + rest, NB))],
            scratch_shapes=[square] * 3,
        ),
        out_shape=[jax.ShapeDtypeStruct((half + rest, width), f32), jax.ShapeDtypeStruct((share + rest, NB), f32)],
        compiler_params=params(1, 32),
        cost_estimate=cost(15e9, 4 << 20),
        name="second_step",
    )(scalars, lp, d1, l0, bp)


def settle(scalars, parts, lower0, share, count):
    half = share // 2
    width = 2 * NB
    tall = lower0.shape[0]
    rest = tall - share

    def body(sc_ref, *refs):
        l0_ref, lh, fixed = refs[-3:]
        low = refs[0][...]
        for ref in refs[1:-3]:
            low = low + ref[...]
        fixed[...] = l0_ref[...]

        @pl.when(sc_ref[0] == 1)
        def _():
            fixed[share:, :] = place(low[half:, NB:width], natural(sc_ref, count, share))

        for n, piece in enumerate(split2(low)):
            at = n * tall
            lh[at : at + half, 0:NB] = piece[0:half, 0:NB]
            lh[at + half : at + share, 0:NB] = piece[0:half, NB:width]
            lh[at : at + share, NB:width] = jnp.zeros((share, NB), bf16)
            lh[at + share : at + tall, :] = piece[half:, :]

    full = lambda shape: pl.BlockSpec(shape, lambda i, sc: (0, 0))
    return pl.pallas_call(
        body,
        grid_spec=pltpu.PrefetchScalarGridSpec(
            num_scalar_prefetch=1,
            grid=(1,),
            in_specs=[full((half + rest, width))] * len(parts) + [full((tall, NB))],
            out_specs=[full((2 * tall, width)), full((tall, NB))],
        ),
        out_shape=[jax.ShapeDtypeStruct((2 * tall, width), bf16), jax.ShapeDtypeStruct((tall, NB), f32)],
        compiler_params=params(1),
        cost_estimate=cost(1e9, 4 * tall * width * (len(parts) + 2)),
        name="settle",
    )(scalars, *parts, lower0)


def came_from(sc, k):
    return sc[0] ^ k


def product(scalars, k, lh, fixed, blocks, share):
    tall = fixed.shape[0]
    rest = tall - share
    piv = 2 * share
    width = 2 * NB
    total = blocks[0].shape[1]
    count = len(blocks)
    piece = NB // 2
    tile = NB
    steps = total // tile

    def body(sc_ref, lh_ref, fixed_ref, *refs):
        b_refs = refs[:count]
        vp_ref, pn_ref = refs[count:]
        for j in range(tile // piece):
            cols = slice(j * piece, (j + 1) * piece)
            raw = [ref[:, cols] for ref in b_refs]
            hi, lo = split2(jnp.concatenate([x[0:share] for x in raw] + [x[share:] for x in raw], axis=0))
            big = dot(lh_ref[...], hi)
            prod = big[0:tall] + (big[tall:] + dot(lh_ref[0:tall, :], lo))
            vp_ref[0:share, cols] = raw[0][0:share]
            vp_ref[share:piv, cols] = raw[0][share:] - prod[0:share]
            pn_ref[:, cols] = prod[share:]

        @pl.when((pl.program_id(0) == 0) & (came_from(sc_ref, k) == 0) & (sc_ref[0] == 0))
        def _():
            vp_ref[share:piv, 0:NB] = fixed_ref[0:share, :]

    full = lambda shape: pl.BlockSpec(shape, lambda i, sc: (0, 0))
    moving = lambda n: pl.BlockSpec((n, tile), lambda i, sc: (0, i))
    return pl.pallas_call(
        body,
        grid_spec=pltpu.PrefetchScalarGridSpec(
            num_scalar_prefetch=1,
            grid=(steps,),
            in_specs=[full((2 * tall, width)), full((tall, NB))] + [moving(piv)] * count,
            out_specs=[moving(piv), moving(rest)],
        ),
        out_shape=[jax.ShapeDtypeStruct((piv, total), f32), jax.ShapeDtypeStruct((rest, total), f32)],
        compiler_params=params(1),
        cost_estimate=cost(6 * tall * width * total, 4 * (width + piv + rest) * total),
        name="product",
    )(scalars, lh, fixed, *blocks)


def finish(scalars, k, st, fixed, done, prod, others, out, out_shape):
    rows = st.shape[0]
    piv = done.shape[0]
    rest = rows - piv
    total = others.shape[1]
    tile = 2 * NB if total % (2 * NB) == 0 else NB
    steps = total // tile
    piece = NB // 2

    def body(sc_ref, st_ref, fixed_ref, d_ref, p_ref, n_ref, *refs):
        o_ref = refs[-1]
        panel = (pl.program_id(0) == 0) & (came_from(sc_ref, k) == 0) & (sc_ref[0] < 2)
        for j in range(tile // piece):
            cols = slice(j * piece, (j + 1) * piece)
            low = n_ref[:, cols] - p_ref[:, cols]
            if (j + 1) * piece <= NB:
                low = jnp.where(panel, fixed_ref[piv // 2 :, cols], low)
            o_ref[:, cols] = select(st_ref[...], jnp.concatenate([d_ref[:, cols], low], axis=0))

    full = lambda shape: pl.BlockSpec(shape, lambda i, sc: (0, 0))
    moving = lambda n: pl.BlockSpec((n, tile), lambda i, sc: (0, i))
    operands = [st, fixed, done, prod, others]
    in_specs = [full((rows, rows)), full((fixed.shape[0], NB)), moving(piv), moving(rest), moving(rest)]
    aliases = {}
    if out is not None:
        aliases = {1 + len(operands): 0}
        operands.append(out)
        in_specs.append(pl.BlockSpec(memory_space=pl.ANY))
    return pl.pallas_call(
        body,
        grid_spec=pltpu.PrefetchScalarGridSpec(
            num_scalar_prefetch=1,
            grid=(steps,),
            in_specs=in_specs,
            out_specs=pl.BlockSpec((rows, tile), lambda i, sc: (0, came_from(sc, k) * steps + i)),
        ),
        out_shape=out_shape,
        input_output_aliases=aliases,
        compiler_params=params(1),
        cost_estimate=cost(6 * rows * rows * total, 4 * (rows + rest) * total),
        name="finish",
    )(scalars, *operands)


def across(x, size, move):
    return lax.ppermute(x, "prow", [(i, move(i)) for i in range(size)])


def gather_rows(x, size):
    blocks = [x]
    if size == 8:
        one = lambda i: i ^ (2 if i % 2 == 0 else 4)
        two = lambda i: i ^ (4 if i % 2 == 0 else 2)
        a = across(x, size, one)
        b = across(x, size, two)
        blocks += [a, b, across(a, size, two)]
    else:
        blocks += [across(x, size, lambda i, m=m: i ^ m) for m in range(2, size, 2)]
    return blocks + [across(block, size, lambda i: i ^ 1) for block in blocks]


def block_ids(row, size):
    even = row % 2 == 0
    if size == 8:
        ids = [row, jnp.where(even, row ^ 2, row ^ 4), jnp.where(even, row ^ 4, row ^ 2), row ^ 6]
        mate = row ^ 1
        ids += [mate, jnp.where(even, mate ^ 4, mate ^ 2), jnp.where(even, mate ^ 2, mate ^ 4), mate ^ 6]
        return ids
    ids = [row ^ m for m in range(0, size, 2)]
    return ids + [i ^ 1 for i in ids]


def on_device(skeleton, pivots):
    rows, local = skeleton.shape
    size = lax.axis_size("prow")
    devs = lax.axis_size("pcol")
    row = lax.axis_index("prow")
    col = lax.axis_index("pcol")
    share = NB // size
    scalars = jnp.stack([col, row] + block_ids(row, size)).astype(jnp.int32)
    own = lax.dynamic_slice_in_dim(pivots, row * share, share, axis=1) - row * rows

    def shift(x, k):
        return lax.ppermute(x, "pcol", [(i, i ^ k) for i in range(devs)])

    def send(x, pairs):
        return lax.ppermute(x, "pcol", pairs)

    order = rotations(devs)
    per = local // NB // devs
    towards = lambda k: [lambda sc, i=i: (sc[0] ^ k) + devs * i for i in range(per)]
    piv_rows = 2 * share
    first, *others = order
    *head, onehot, st = pick(scalars, None, skeleton, towards(first), piv_rows, own)
    picked = {first: head}
    for k in others + [0]:
        picked[k] = pick(scalars, onehot, skeleton, towards(k), piv_rows)
    panel_piv, panel_rest = pick(scalars, onehot, skeleton, [lambda sc: 0, lambda sc: 1], piv_rows)
    piv = {k: shift(picked[k][0], k) if k else picked[k][0] for k in [0] + order}
    panel = gather_rows(panel_piv, size)
    lp, d1, l0, bp = first_step(scalars, panel, panel_rest, share)
    lower, lower0 = second_step(scalars, lp, d1, l0, bp, share)
    reach = devs // 2
    moved = send(lower, [(0, reach)])
    parts = [lower, moved]
    while reach > 1:
        reach //= 2
        direct = send(lower, [(0, reach)])
        onward = send(moved, [(i, i + reach) for i in range(2 * reach, devs, 2 * reach)])
        parts += [direct, onward]
        moved = moved + direct + onward if reach > 1 else moved
    rest = {k: shift(picked[k][1], k) if k else picked[k][1] for k in [0] + order}
    lh, fixed = settle(scalars, parts, lower0, share, len(panel))
    shape = jax.ShapeDtypeStruct((rows, local), f32)
    ready = {}
    for k in [0] + order:
        blocks = gather_rows(piv[k], size)
        ready[k] = product(scalars, k, lh, fixed, blocks, share)
    out = None
    for k in [0] + order:
        out = finish(scalars, k, st, fixed, *ready[k], rest[k], out, shape)
    return out


def rotations(devs):
    return sorted(range(1, devs), key=lambda k: (k != devs - 1, k))


def solution(mesh):
    placed = (P("prow", "pcol"), P())
    return jax.shard_map(on_device, mesh=mesh, in_specs=placed, out_specs=P("prow", "pcol"), check_vma=False)
```

```python
import jax
import jax.numpy as jnp
from jax import lax
from jax.experimental import pallas as pl
from jax.experimental.pallas import tpu as pltpu
from jax.sharding import PartitionSpec as P

NB = 512
f32 = jnp.float32
bf16 = jnp.bfloat16
highest = lax.Precision.HIGHEST


def dot(a, b):
    return jnp.dot(a, b, preferred_element_type=f32)


def split2(x):
    hi = x.astype(bf16)
    return hi, (x - hi.astype(f32)).astype(bf16)


def dot3(a, b):
    ah, al = split2(a)
    bh, bl = split2(b)
    return dot(ah, bh) + (dot(ah, bl) + dot(al, bh))


def dot6(a, b):
    return jnp.dot(a, b, preferred_element_type=f32, precision=highest)


def select(onehot, x):
    y = x * 0.5
    hi = y.astype(bf16)
    rest = y - hi.astype(f32)
    mid = rest.astype(bf16)
    low = (rest - mid.astype(f32)).astype(bf16)
    return 2.0 * ((dot(onehot, hi) + dot(onehot, mid)) + dot(onehot, low))


def cost(flops, nbytes):
    return pl.CostEstimate(flops=int(flops), transcendentals=0, bytes_accessed=int(nbytes))


def params(n, mib=20):
    return pltpu.CompilerParams(dimension_semantics=("arbitrary",) * n, vmem_limit_bytes=mib << 20)


def pick(onehot, skeleton, columns, piv, grant, pivots=None):
    rows = skeleton.shape[0]
    rest = rows - piv
    per = len(columns)
    make = pivots is not None

    def order(pivots_ref, s_ref, st_ref):
        share = piv // 2
        row = lax.axis_index("prow")
        line = lax.broadcasted_iota(jnp.int32, (rows, NB), 0) + row * rows
        entry = lax.broadcasted_iota(jnp.int32, (NB, share), 0) - lax.broadcasted_iota(jnp.int32, (NB, share), 1)
        mine = (entry == row * share).astype(f32).astype(bf16)
        hits = [(line == pivots_ref[t : t + 1, :]).astype(f32).astype(bf16) for t in range(2)]
        sp = jnp.concatenate([dot(hit, mine) for hit in hits], axis=1).T
        free = 1.0 - jnp.sum(sp, axis=0, keepdims=True)
        before = lax.broadcasted_iota(jnp.int32, (rows, rows), 0) < lax.broadcasted_iota(jnp.int32, (rows, rows), 1)
        rank = dot(jnp.broadcast_to(free, (8, rows)).astype(bf16), before.astype(f32).astype(bf16))[0:1]
        place_of = lax.broadcasted_iota(jnp.int32, (rest, rows), 0).astype(f32)
        full_order = jnp.concatenate([sp, jnp.where(rank == place_of, free, 0.0)], axis=0)
        st_ref[...] = full_order.T.astype(bf16)
        s_ref[...] = full_order.astype(bf16)

    def body(s_in, x_hbm, *refs):
        piv_ref, rest_ref = refs[:2]
        blocks, sems = refs[-2:]
        col = lax.axis_index("pcol")
        copies = []
        for i, at in enumerate(columns):
            start = pl.multiple_of(at(col) * NB, NB)
            copies.append(pltpu.make_async_copy(x_hbm.at[:, pl.ds(start, NB)], blocks.at[i], sems.at[i]))
            copies[-1].start()
        if make:
            order(s_in, *refs[2:4])
            s_in = refs[2]
        for i, copy in enumerate(copies):
            copy.wait()
            x = select(s_in[...], blocks[i])
            piv_ref[:, i * NB : (i + 1) * NB] = x[0:piv]
            rest_ref[:, i * NB : (i + 1) * NB] = x[piv:]

    whole = lambda shape: pl.BlockSpec(shape, lambda _: (0, 0))
    shapes = [((piv, per * NB), f32), ((rest, per * NB), f32)] + [((rows, rows), bf16)] * (2 if make else 0)
    source = pivots if make else onehot
    return pl.pallas_call(
        body,
        grid=(1,),
        in_specs=[whole(source.shape), pl.BlockSpec(memory_space=pltpu.MemorySpace.HBM)],
        out_specs=[whole(x) for x, _ in shapes],
        out_shape=[jax.ShapeDtypeStruct(x, d) for x, d in shapes],
        scratch_shapes=[pltpu.VMEM((per, rows, NB), f32), pltpu.SemaphoreType.DMA((per,))],
        compiler_params=params(1, grant),
        cost_estimate=cost(6 * rows * rows * per * NB, 8 * rows * per * NB),
        name="pick",
    )(source, skeleton)


def invert(d_ref, x_ref, r_ref):
    n = d_ref.shape[0]
    eye = lax.broadcasted_iota(jnp.int32, (n, n), 0) == lax.broadcasted_iota(jnp.int32, (n, n), 1)

    def total(v):
        return jnp.sum(jnp.sum(v, axis=0, keepdims=True), axis=1, keepdims=True)

    d = d_ref[...]
    size = jnp.max(jnp.max(jnp.abs(d), axis=0, keepdims=True), axis=1, keepdims=True)
    unit = 1.0 / size
    d = d * unit
    d_ref[...] = d
    dh = d.astype(bf16)
    power = lax.dot_general(dh, dh, (((1,), (1,)), ((), ())), preferred_element_type=f32)
    norm = jnp.sqrt(total(power * power))
    norms = [norm]
    for _ in range(3):
        ph = (power * (1.0 / norm)).astype(bf16)
        power = dot(ph, ph)
        norm = jnp.sqrt(total(power * power))
        norms.append(norm)
    bound = norms[-1]
    for value in reversed(norms[:-1]):
        bound = value * jnp.sqrt(bound)
    x_ref[...] = d.T * (1.7 / bound)

    def residual(product):
        r = jnp.where(eye, 1.0, 0.0) - product
        r_ref[...] = r
        return jnp.sum(r * r)

    def coarse(carry):
        x = x_ref[...]
        x_ref[...] = x + dot(x.astype(bf16), r_ref[...].astype(bf16))
        return carry[0] + 1, residual(dot(d_ref[...].astype(bf16), x_ref[...].astype(bf16)))

    def fine(carry):
        x = x_ref[...]
        x_ref[...] = x + dot3(x, r_ref[...])
        return carry[0] + 1, residual(dot3(d_ref[...], x_ref[...]))

    first = residual(dot(d_ref[...].astype(bf16), x_ref[...].astype(bf16)))
    done = lax.while_loop(lambda c: (c[1] > 1.0) & (c[0] < 24), coarse, (jnp.int32(0), first))
    start = residual(dot3(d_ref[...], x_ref[...]))
    lax.while_loop(lambda c: (c[1] > 4e-6) & (c[0] < 24), fine, (done[0] * 0, start))
    residual(dot6(d_ref[...], x_ref[...]))
    x = x_ref[...]
    x_ref[...] = (x + dot3(x, r_ref[...])) * unit


def natural(sc_ref, count, share):
    n = count * share
    at = lax.broadcasted_iota(jnp.int32, (share, n), 1) - lax.broadcasted_iota(jnp.int32, (share, n), 0)
    return jnp.concatenate([(at == sc_ref[2 + m] * share).astype(f32) for m in range(count)], axis=0).astype(bf16)


def place(x, onehot):
    y = x * 0.5
    hi = y.astype(bf16)
    rest = y - hi.astype(f32)
    mid = rest.astype(bf16)
    low = (rest - mid.astype(f32)).astype(bf16)
    return 2.0 * ((dot(hi, onehot) + dot(mid, onehot)) + dot(low, onehot))


def first_step(scalars, blocks, panel_rest, share):
    rest = panel_rest.shape[0]
    width = 2 * NB
    count = len(blocks)

    def body(sc_ref, *refs):
        b_refs = refs[:count]
        pn_ref, lp, d1, l0, bp, w0, w1, d_ref, x0, r_ref = refs[count:]

        @pl.when(sc_ref[0] == 0)
        def _():
            for m in range(count):
                w0[m * share : (m + 1) * share, :] = b_refs[m][0:share, :]
                w1[m * share : (m + 1) * share, :] = b_refs[m][share : 2 * share, :]
            d_ref[...] = w0[:, 0:NB]
            invert(d_ref, x0, r_ref)
            low = dot3(w1[:, 0:NB], x0[...])
            lp[...] = low
            d1[...] = w1[:, NB:width] - dot3(low, w0[:, NB:width])
            mine = dot3(pn_ref[:, 0:NB], x0[...])
            l0[...] = mine
            bp[...] = pn_ref[:, NB:width] - dot3(mine, w0[:, NB:width])

    full = lambda shape: pl.BlockSpec(shape, lambda i, sc: (0, 0))
    square = pltpu.VMEM((NB, NB), f32)
    shapes = [(NB, NB), (NB, NB), (rest, NB), (rest, NB)]
    return pl.pallas_call(
        body,
        grid_spec=pltpu.PrefetchScalarGridSpec(
            num_scalar_prefetch=1,
            grid=(1,),
            in_specs=[full((2 * share, width))] * count + [full((rest, width))],
            out_specs=[full(x) for x in shapes],
            scratch_shapes=[pltpu.VMEM((NB, width), f32)] * 2 + [square] * 3,
        ),
        out_shape=[jax.ShapeDtypeStruct(x, f32) for x in shapes],
        compiler_params=params(1, 32),
        cost_estimate=cost(20e9, 8 << 20),
        name="first_step",
    )(scalars, *blocks, panel_rest)


def second_step(scalars, lp, d1, l0, bp, share):
    rest = l0.shape[0]
    half = share // 2
    width = 2 * NB
    count = NB // share

    def body(sc_ref, lp_ref, d1_ref, l0_in, bp_ref, l_ref, l0_ref, d_ref, x1, r_ref):
        @pl.when(sc_ref[0] != 0)
        def _():
            l_ref[...] = jnp.zeros_like(l_ref)
            l0_ref[...] = jnp.zeros_like(l0_ref)

        @pl.when(sc_ref[0] == 0)
        def _():
            d_ref[...] = d1_ref[...]
            invert(d_ref, x1, r_ref)
            l1 = dot3(bp_ref[...], x1[...])
            l_ref[half:, 0:NB] = l0_in[...] - dot3(l1, lp_ref[...])
            l_ref[half:, NB:width] = l1
            l_ref[0:half, 0:NB] = lp_ref[0:half, :]
            l_ref[0:half, NB:width] = lp_ref[half:share, :]
            back = natural(sc_ref, count, share)
            l0_ref[0:share, :] = place(lp_ref[0:share, :], back)
            l0_ref[share:, :] = place(l0_in[...], back)

    full = lambda shape: pl.BlockSpec(shape, lambda i, sc: (0, 0))
    square = pltpu.VMEM((NB, NB), f32)
    return pl.pallas_call(
        body,
        grid_spec=pltpu.PrefetchScalarGridSpec(
            num_scalar_prefetch=1,
            grid=(1,),
            in_specs=[full((NB, NB)), full((NB, NB)), full((rest, NB)), full((rest, NB))],
            out_specs=[full((half + rest, width)), full((share + rest, NB))],
            scratch_shapes=[square] * 3,
        ),
        out_shape=[jax.ShapeDtypeStruct((half + rest, width), f32), jax.ShapeDtypeStruct((share + rest, NB), f32)],
        compiler_params=params(1, 32),
        cost_estimate=cost(15e9, 4 << 20),
        name="second_step",
    )(scalars, lp, d1, l0, bp)


def settle(scalars, parts, lower0, share, count):
    half = share // 2
    width = 2 * NB
    tall = lower0.shape[0]
    rest = tall - share

    def body(sc_ref, *refs):
        l0_ref, lh, fixed = refs[-3:]
        low = refs[0][...]
        for ref in refs[1:-3]:
            low = low + ref[...]
        fixed[...] = l0_ref[...]

        @pl.when(sc_ref[0] == 1)
        def _():
            fixed[share:, :] = place(low[half:, NB:width], natural(sc_ref, count, share))

        for n, piece in enumerate(split2(low)):
            at = n * tall
            lh[at : at + half, 0:NB] = piece[0:half, 0:NB]
            lh[at + half : at + share, 0:NB] = piece[0:half, NB:width]
            lh[at : at + share, NB:width] = jnp.zeros((share, NB), bf16)
            lh[at + share : at + tall, :] = piece[half:, :]

    full = lambda shape: pl.BlockSpec(shape, lambda i, sc: (0, 0))
    return pl.pallas_call(
        body,
        grid_spec=pltpu.PrefetchScalarGridSpec(
            num_scalar_prefetch=1,
            grid=(1,),
            in_specs=[full((half + rest, width))] * len(parts) + [full((tall, NB))],
            out_specs=[full((2 * tall, width)), full((tall, NB))],
        ),
        out_shape=[jax.ShapeDtypeStruct((2 * tall, width), bf16), jax.ShapeDtypeStruct((tall, NB), f32)],
        compiler_params=params(1),
        cost_estimate=cost(1e9, 4 * tall * width * (len(parts) + 2)),
        name="settle",
    )(scalars, *parts, lower0)


def came_from(sc, k):
    return sc[0] ^ k


def product(scalars, k, lh, fixed, blocks, share):
    tall = fixed.shape[0]
    rest = tall - share
    piv = 2 * share
    width = 2 * NB
    total = blocks[0].shape[1]
    count = len(blocks)
    piece = NB // 2
    tile = NB
    steps = total // tile

    def body(sc_ref, lh_ref, fixed_ref, *refs):
        b_refs = refs[:count]
        vp_ref, pn_ref = refs[count:]
        for j in range(tile // piece):
            cols = slice(j * piece, (j + 1) * piece)
            raw = [ref[:, cols] for ref in b_refs]
            hi, lo = split2(jnp.concatenate([x[0:share] for x in raw] + [x[share:] for x in raw], axis=0))
            big = dot(lh_ref[...], hi)
            prod = big[0:tall] + (big[tall:] + dot(lh_ref[0:tall, :], lo))
            vp_ref[0:share, cols] = raw[0][0:share]
            vp_ref[share:piv, cols] = raw[0][share:] - prod[0:share]
            pn_ref[:, cols] = prod[share:]

        @pl.when((pl.program_id(0) == 0) & (came_from(sc_ref, k) == 0) & (sc_ref[0] == 0))
        def _():
            vp_ref[share:piv, 0:NB] = fixed_ref[0:share, :]

    full = lambda shape: pl.BlockSpec(shape, lambda i, sc: (0, 0))
    moving = lambda n: pl.BlockSpec((n, tile), lambda i, sc: (0, i))
    return pl.pallas_call(
        body,
        grid_spec=pltpu.PrefetchScalarGridSpec(
            num_scalar_prefetch=1,
            grid=(steps,),
            in_specs=[full((2 * tall, width)), full((tall, NB))] + [moving(piv)] * count,
            out_specs=[moving(piv), moving(rest)],
        ),
        out_shape=[jax.ShapeDtypeStruct((piv, total), f32), jax.ShapeDtypeStruct((rest, total), f32)],
        compiler_params=params(1),
        cost_estimate=cost(6 * tall * width * total, 4 * (width + piv + rest) * total),
        name="product",
    )(scalars, lh, fixed, *blocks)


def finish(scalars, k, st, fixed, done, prod, others, out, out_shape):
    rows = st.shape[0]
    piv = done.shape[0]
    rest = rows - piv
    total = others.shape[1]
    tile = 2 * NB if total % (2 * NB) == 0 else NB
    steps = total // tile
    piece = NB // 2

    def body(sc_ref, st_ref, fixed_ref, d_ref, p_ref, n_ref, *refs):
        o_ref = refs[-1]
        panel = (pl.program_id(0) == 0) & (came_from(sc_ref, k) == 0) & (sc_ref[0] < 2)
        for j in range(tile // piece):
            cols = slice(j * piece, (j + 1) * piece)
            low = n_ref[:, cols] - p_ref[:, cols]
            if (j + 1) * piece <= NB:
                low = jnp.where(panel, fixed_ref[piv // 2 :, cols], low)
            o_ref[:, cols] = select(st_ref[...], jnp.concatenate([d_ref[:, cols], low], axis=0))

    full = lambda shape: pl.BlockSpec(shape, lambda i, sc: (0, 0))
    moving = lambda n: pl.BlockSpec((n, tile), lambda i, sc: (0, i))
    operands = [st, fixed, done, prod, others]
    in_specs = [full((rows, rows)), full((fixed.shape[0], NB)), moving(piv), moving(rest), moving(rest)]
    aliases = {}
    if out is not None:
        aliases = {1 + len(operands): 0}
        operands.append(out)
        in_specs.append(pl.BlockSpec(memory_space=pl.ANY))
    return pl.pallas_call(
        body,
        grid_spec=pltpu.PrefetchScalarGridSpec(
            num_scalar_prefetch=1,
            grid=(steps,),
            in_specs=in_specs,
            out_specs=pl.BlockSpec((rows, tile), lambda i, sc: (0, came_from(sc, k) * steps + i)),
        ),
        out_shape=out_shape,
        input_output_aliases=aliases,
        compiler_params=params(1),
        cost_estimate=cost(6 * rows * rows * total, 4 * (rows + rest) * total),
        name="finish",
    )(scalars, *operands)


def across(x, size, move):
    return lax.ppermute(x, "prow", [(i, move(i)) for i in range(size)])


def gather_rows(x, size):
    blocks = [x]
    if size == 8:
        one = lambda i: i ^ (2 if i % 2 == 0 else 4)
        two = lambda i: i ^ (4 if i % 2 == 0 else 2)
        a = across(x, size, one)
        b = across(x, size, two)
        blocks += [a, b, across(a, size, two)]
    else:
        blocks += [across(x, size, lambda i, m=m: i ^ m) for m in range(2, size, 2)]
    return blocks + [across(block, size, lambda i: i ^ 1) for block in blocks]


def block_ids(row, size):
    even = row % 2 == 0
    if size == 8:
        ids = [row, jnp.where(even, row ^ 2, row ^ 4), jnp.where(even, row ^ 4, row ^ 2), row ^ 6]
        mate = row ^ 1
        ids += [mate, jnp.where(even, mate ^ 4, mate ^ 2), jnp.where(even, mate ^ 2, mate ^ 4), mate ^ 6]
        return ids
    ids = [row ^ m for m in range(0, size, 2)]
    return ids + [i ^ 1 for i in ids]


def on_device(skeleton, pivots):
    rows, local = skeleton.shape
    size = lax.axis_size("prow")
    devs = lax.axis_size("pcol")
    row = lax.axis_index("prow")
    col = lax.axis_index("pcol")
    share = NB // size
    scalars = jnp.stack([col, row] + block_ids(row, size)).astype(jnp.int32)

    def shift(x, k):
        return lax.ppermute(x, "pcol", [(i, i ^ k) for i in range(devs)])

    def send(x, pairs):
        return lax.ppermute(x, "pcol", pairs)

    order = rotations(devs)
    per = local // NB // devs
    towards = lambda k: [lambda col, i=i: (col ^ k) + devs * i for i in range(per)]
    piv_rows = 2 * share
    first, *others = order
    *head, onehot, st = pick(None, skeleton, towards(first), piv_rows, 56, pivots)
    picked = {first: head}
    panel_piv, panel_rest = pick(onehot, skeleton, [lambda col: 0, lambda col: 1], piv_rows, 54)
    for n, k in enumerate(others + [0]):
        picked[k] = pick(onehot, skeleton, towards(k), piv_rows, max(52 - 2 * n, 48))
    piv = {k: shift(picked[k][0], k) if k else picked[k][0] for k in [0] + order}
    panel = gather_rows(panel_piv, size)
    lp, d1, l0, bp = first_step(scalars, panel, panel_rest, share)
    lower, lower0 = second_step(scalars, lp, d1, l0, bp, share)
    reach = devs // 2
    moved = send(lower, [(0, reach)])
    parts = [lower, moved]
    while reach > 1:
        reach //= 2
        direct = send(lower, [(0, reach)])
        onward = send(moved, [(i, i + reach) for i in range(2 * reach, devs, 2 * reach)])
        parts += [direct, onward]
        moved = moved + direct + onward if reach > 1 else moved
    rest = {k: shift(picked[k][1], k) if k else picked[k][1] for k in [0] + order}
    lh, fixed = settle(scalars, parts, lower0, share, len(panel))
    shape = jax.ShapeDtypeStruct((rows, local), f32)
    ready = {}
    for k in [0] + order:
        blocks = gather_rows(piv[k], size)
        ready[k] = product(scalars, k, lh, fixed, blocks, share)
    out = None
    for k in [0] + order:
        out = finish(scalars, k, st, fixed, *ready[k], rest[k], out, shape)
    return out


def rotations(devs):
    return sorted(range(1, devs), key=lambda k: (k != devs - 1, k))


def solution(mesh):
    placed = (P("prow", "pcol"), P())
    return jax.shard_map(on_device, mesh=mesh, in_specs=placed, out_specs=P("prow", "pcol"), check_vma=False)
```
